512 devices in a mesh: state: 8 (over y_lo, x), bond: 64 (over z, y_hi, core).
Axes of the slice: x: 4, y: 8 (y_hi: 4, y_lo: 2; y = y_hi * 2 + y_lo), z: 8, core: 2. Of those that a mesh axis runs over, the one named last changes fastest.
Arguments:
- intersect_left: bfloat16 [8, 2048, 2048], P('state', 'bond'), may hold values from -0.125 to 0.125
- stored_block: bfloat16 [8, 4, 2048, 2048], P('state', None, 'bond'), may hold values from -6 to 6
- stored_site: bfloat16 [8, 2, 2048, 2048], P('state', None, 'bond'), may hold values from -6 to 6
- current_site: bfloat16 [2048, 2, 2048], P('bond', None, 'state'), may hold values from -0.09375 to 0.09375
- current_block: bfloat16 [4, 2048, 2048], P(None, 'bond', 'state'), may hold values from -6 to 6
- penalty_weight: float32 [8], replicated, may hold values from 0.5 to 4
Outputs:
- penalized: float32 [4, 2048, 2048], P(None, 'bond', 'state')
- intersect_next: bfloat16 [8, 2048, 2048], P('state', 'bond')
The draws below stay inside these ranges and needn't reach their ends.
All inputs are finite; a program needn't handle non-finite values.
Results may differ from the reference program's by a relative error of at most 0.0055.
Values may be sent and summed in bfloat16 or wider, within the bound.
No kernel may reach another device: no remote copies, remote signals or barrier semaphores. Data moves between devices by JAX's collectives and lax.ppermute only.
A program may use at most 64 MiB of HBM per device.

```python
import math
import jax
import jax.numpy as jnp

D = 2048
PHYS = 2
Q = 4
STATES = 8


def level_of(rng, dims, pieces, least, high):
    def one(axis_at, shards_of):
        draws = jax.random.uniform(jax.random.fold_in(jax.random.fold_in(rng, 6), axis_at), (shards_of,), jnp.float32, least / len(pieces), high / len(pieces))
        return jnp.repeat(jnp.exp(draws), dims[axis_at] // shards_of).reshape((-1,) + (1,) * (len(dims) - axis_at - 1))

    factor_of = one(*pieces[0])
    for cut in pieces[1:]:
        factor_of = factor_of * one(*cut)
    return factor_of


def normal_values(key, dims, scale, limit, split=(), kind=jnp.bfloat16):
    result = scale * jax.random.normal(key, dims, jnp.float32)
    if split:
        result = result * level_of(key, dims, split, -0.22, 0.18)
    return jnp.clip(result, -limit, limit).astype(kind)


def setup_inputs(seed: int = 0) -> dict:
    seeds = jax.random.split(jax.random.key(seed), 7)
    return {
        "intersect_left": normal_values(seeds[0], (STATES, D, D), D ** -0.5, 0.125, ((0, 8), (1, 64))),
        "stored_block": normal_values(seeds[1], (STATES, Q, D, D), 1.0, 6.0, ((0, 8), (2, 64))),
        "stored_site": normal_values(seeds[2], (STATES, PHYS, D, D), 1.0, 6.0, ((0, 8), (2, 64))),
        "current_site": normal_values(seeds[3], (D, PHYS, D), (PHYS * D) ** -0.5, 0.09375, ((0, 64), (2, 8))),
        "current_block": normal_values(seeds[4], (Q, D, D), 1.0, 6.0, ((1, 64), (2, 8))),
        "penalty_weight": jnp.clip(jnp.exp(jax.random.uniform(seeds[5], (STATES,), jnp.float32, math.log(0.5), math.log(4.0))), 0.5, 4.0),
    }


def reference(intersect_left, stored_block, stored_site, current_site, current_block, penalty_weight):
    block_wide = current_block.astype(jnp.float32)
    site_wide = current_site.astype(jnp.float32)
    penalized = block_wide
    grown_list = []
    for index in range(STATES):
        env_turned = intersect_left[index].T
        projected = jnp.dot(stored_block[index].reshape(Q * D, D), env_turned, preferred_element_type=jnp.float32).reshape(Q, D, D)
        intersect = jnp.sum(projected * block_wide) / (PHYS * D)
        penalized = penalized + (penalty_weight[index] * intersect) * projected
        moved = jnp.dot(stored_site[index].reshape(PHYS * D, D), env_turned, preferred_element_type=jnp.float32).astype(jnp.bfloat16)
        moved = moved.reshape(PHYS, D, D).astype(jnp.float32)
        grown = jnp.einsum("asf,sea->fe", site_wide, moved).astype(jnp.bfloat16)
        grown_list.append(grown)
    return penalized, jnp.stack(grown_list)
```

```python
import jax
import jax.numpy as jnp
from jax import lax
from jax.sharding import Mesh
from jax.sharding import PartitionSpec as P

STATE = ("state_0", "state_1")
ROW = "bond_0"
COLUMN = "bond_1"
CORE = "bond_2"


def shifted(value, axis, step):
    size = lax.axis_size(axis)
    return lax.ppermute(value, axis, [(i, (i + step) % size) for i in range(size)])


def sent_to_all(value, axis):
    copies = jnp.broadcast_to(value, (lax.axis_size(axis), *value.shape))
    return lax.all_to_all(copies, axis, split_axis=0, concat_axis=0, tiled=True)


def placed(pieces, places):
    first = pieces[0]
    whole = jnp.zeros((len(pieces), *first.shape), first.dtype)
    for piece, place in zip(pieces, places):
        whole = lax.dynamic_update_slice(whole, piece[None], (place,) + (0,) * first.ndim)
    return whole


def ring_of_four(value, axis):
    here = lax.axis_index(axis)
    half = value.shape[0] // 2
    below = shifted(value, axis, 1)
    above = shifted(value, axis, -1)
    far = jnp.concatenate([shifted(below[:half], axis, 1), shifted(above[half:], axis, -1)], axis=0)
    return placed([value, below, above, far], [here, (here + 3) % 4, (here + 1) % 4, (here + 2) % 4])


def with_partner(value):
    other = shifted(value, CORE, 1)
    first = lax.axis_index(CORE) == 0
    return jnp.where(first, jnp.stack([value, other]), jnp.stack([other, value]))


def rows_times(left, right):
    return lax.dot_general(left, right, (((1,), (1,)), ((), ())), preferred_element_type=jnp.float32)


def shards(intersect_left, stored_block, stored_site, current_site, current_block, penalty_weight):
    states = lax.axis_size(STATE)
    rows = lax.axis_size(ROW)
    columns = lax.axis_size(COLUMN)
    pairs, width, bond = stored_block.shape[1:]
    physical = stored_site.shape[1]
    block = current_block.shape[2]
    half = block // 2
    z = lax.axis_index(ROW)

    environment = ring_of_four(intersect_left[0], COLUMN).reshape(columns * width, bond)

    blocks_two = with_partner(stored_block[0])
    site_four = ring_of_four(stored_site[0].reshape(physical * width, bond), COLUMN)
    site_all = with_partner(site_four.reshape(columns, physical, width, bond))
    site_all = site_all.transpose(2, 1, 0, 3, 4).reshape(physical * block, bond)
    block_rows = 2 * pairs * width
    operand = jnp.concatenate([blocks_two.reshape(block_rows, bond), site_all], axis=0)

    part = block // columns
    site = current_site.reshape(width, physical, columns, part).transpose(2, 0, 1, 3)
    site = site.reshape(columns, width, physical * part)
    site = lax.all_to_all(site, COLUMN, 0, 0, tiled=True).reshape(columns * width, physical * part)
    site = sent_to_all(sent_to_all(site, ROW), STATE)

    apart = current_block.reshape(pairs, width, columns, 2, width)
    apart = apart.transpose(3, 0, 1, 2, 4).reshape(2, pairs, width, half)
    current = jnp.broadcast_to(apart, (states, *apart.shape)).reshape(states * 2, pairs, width, half)
    current = lax.all_to_all(current, (*STATE, CORE), 0, 0, tiled=True)
    current = current.reshape(states, 2, pairs, width, half)

    projected = []
    moved = []
    overlap = []
    offsets = []

    def use(piece, offset):
        product = rows_times(operand, piece)
        one = product[:block_rows].reshape(2, pairs, width, half)
        place = (z + offset) % rows
        seen = lax.dynamic_index_in_dim(current, place, 0, keepdims=False)
        overlap.append(jnp.sum(one * seen.astype(jnp.float32)))
        projected.append(one.astype(jnp.bfloat16))
        moved.append(product[block_rows:].astype(jnp.bfloat16))
        offsets.append(place)

    use(environment, 0)
    below = above = environment
    for step in range(1, rows // 2):
        below = shifted(below, ROW, 1)
        above = shifted(above, ROW, -1)
        use(below, rows - step)
        use(above, step)
    split = environment.shape[0] // 2
    far = jnp.concatenate([shifted(below[:split], ROW, 1), shifted(above[split:], ROW, -1)], axis=0)
    use(far, rows // 2)

    sent = placed(projected, offsets).reshape(states * 2, pairs, width, half)
    received = lax.all_to_all(sent, (*STATE, CORE), 0, 0, tiled=True)
    received = received.reshape(states, 2, pairs, width, half)

    scale_factor = 1.0 / (physical * bond)
    total = jnp.full((1, 128), sum(overlap) * scale_factor, jnp.float32)
    total = sent_to_all(total, ROW).sum(axis=0)
    total = sent_to_all(total, (COLUMN, CORE)).sum(axis=0)
    intersect = sent_to_all(total, STATE)[:, 0, 0]
    gain = penalty_weight * intersect
    summed = jnp.sum(gain[:, None, None, None, None] * received.astype(jnp.float32), axis=0)
    summed = summed.reshape(2, pairs, width, columns, width).transpose(1, 2, 3, 0, 4)
    penalized = current_block.astype(jnp.float32) + summed.reshape(pairs, width, block)

    order = jnp.stack(offsets)
    turned = jnp.take(site, order, axis=1).reshape(states, rows * half, physical * part)
    joined = jnp.concatenate(moved, axis=1)
    crossed = lax.dot_general(
        turned, joined, (((1,), (1,)), ((), ())), preferred_element_type=jnp.float32
    )
    grown = crossed[:, :part, :block]
    for s in range(1, physical):
        grown = grown + crossed[:, s * part : (s + 1) * part, s * block : (s + 1) * block]
    grown = grown.astype(jnp.bfloat16).reshape(states * 2, width, block)
    grown = lax.all_to_all(grown, (ROW, CORE), 0, 0, tiled=True).reshape(rows, 2, width, block)
    grown = jnp.sum(grown.astype(jnp.float32), axis=1).astype(jnp.bfloat16)
    intersect_next = grown.transpose(1, 0, 2).reshape(1, width, rows * block)
    return (penalized, intersect_next)


def solution(mesh):
    torus = Mesh(
        mesh.devices.reshape(2, mesh.shape["state"] // 2, 8, 4, 2),
        ("state_0", "state_1", "bond_0", "bond_1", "bond_2"),
    )
    bond = (ROW, COLUMN, CORE)
    in_specs = (
        P(STATE, bond, None),
        P(STATE, None, bond, None),
        P(STATE, None, bond, None),
        P(bond, None, STATE),
        P(None, bond, STATE),
        P(),
    )
    out_specs = (P(None, bond, STATE), P(STATE, bond, None))
    return jax.shard_map(
        shards, mesh=torus, in_specs=in_specs, out_specs=out_specs, check_vma=False
    )
```

```python
import jax
import jax.numpy as jnp
from jax import lax
from jax.experimental import pallas as pl
from jax.experimental.pallas import tpu as pltpu
from jax.sharding import Mesh
from jax.sharding import PartitionSpec as P

STATE = ("state_0", "state_1")
ROW = "bond_0"
FAR = "bond_1"
NEAR = "bond_2"
CORE = "bond_3"


def shifted(value, axis, step):
    size = lax.axis_size(axis)
    return lax.ppermute(value, axis, [(i, (i + step) % size) for i in range(size)])


def exchanged(value, axis):
    return lax.all_to_all(value, axis, split_axis=0, concat_axis=0, tiled=True)


def sent_to_all(value, axis):
    return exchanged(jnp.broadcast_to(value, (lax.axis_size(axis), *value.shape)), axis)


def after(value, *others):
    return lax.optimization_barrier((value, *others))[0]


def load_environment(pieces, environment, semaphores):
    rows = environment.shape[0]
    z = lax.axis_index(ROW)
    copies = []

    def load(piece, offset, target=None):
        place = environment.at[lax.rem(z + offset, rows)]
        if target is not None:
            place = place.at[target]
        copies.append(pltpu.make_async_copy(piece, place, semaphores.at[len(copies)]))

    *whole, low, high = pieces
    load(whole[0], 0)
    for step in range(1, rows // 2):
        load(whole[2 * step - 1], rows - step)
        load(whole[2 * step], step)
    split = low.shape[0]
    load(low, rows // 2, pl.ds(0, split))
    load(high, rows // 2, pl.ds(split, split))
    for copy in copies:
        copy.start()
    return copies


def rows_times(left, right):
    return lax.dot_general(left, right, (((1,), (1,)), ((), ())), preferred_element_type=jnp.float32)


def project_kernel(*refs):
    pieces = refs[:9]
    stored = refs[9:13]
    current, out, overlap, environment, operand, semaphores = refs[13:]
    v = lax.axis_index(NEAR)
    c = lax.axis_index(CORE)
    copies = []
    for k, (flip_v, flip_c) in enumerate(((0, 0), (1, 0), (0, 1), (1, 1))):
        slot = lax.rem(v + flip_v, 2) * 2 + lax.rem(c + flip_c, 2)
        copies.append(pltpu.make_async_copy(stored[k], operand.at[slot], semaphores.at[9 + k]))
        copies[-1].start()
    copies += load_environment(pieces, environment, semaphores)
    for copy in copies:
        copy.wait()
    slots, count, bond = operand.shape
    right = operand[...].reshape(slots * count, bond)
    rows, height, _ = environment.shape
    total = jnp.zeros((height, count), jnp.float32)
    for z in range(0, rows, 2):
        left = environment[z : z + 2].reshape(2 * height, bond)
        product = rows_times(left, right)
        for i in range(2):
            for k in range(slots):
                one = product[i * height : (i + 1) * height, k * count : (k + 1) * count]
                out[z + i, k] = one.astype(jnp.bfloat16)
                total += one * current[z + i, k].astype(jnp.float32)
    overlap[...] = jnp.full(overlap.shape, jnp.sum(total), jnp.float32)


def grow_kernel(*refs):
    pieces = refs[:9]
    mine, other, site, out, environment, operand, moved, semaphores = refs[9:]
    y = lax.axis_index(FAR) * 2 + lax.axis_index(NEAR)
    c = lax.axis_index(CORE)
    copies = load_environment(pieces, environment, semaphores)
    number = len(copies)
    for k, offset in enumerate((0, 3, 1, 2)):
        for flip, source in enumerate((mine, other)):
            slot = lax.rem(y + offset, 4) * 2 + lax.rem(c + flip, 2)
            for s in range(operand.shape[0]):
                copy = pltpu.make_async_copy(
                    source.at[k, s], operand.at[s, slot], semaphores.at[number]
                )
                copy.start()
                copies.append(copy)
                number += 1
    for copy in copies:
        copy.wait()
    physical, slots, count, bond = operand.shape
    block = slots * count
    right = operand[...].reshape(physical * block, bond)
    rows, height, _ = environment.shape
    for z in range(0, rows, 2):
        left = environment[z : z + 2].reshape(2 * height, bond)
        moved[z * height : (z + 2) * height] = rows_times(left, right).astype(jnp.bfloat16)
    for k in range(out.shape[0]):
        total = jnp.zeros(out.shape[1:], jnp.float32)
        for s in range(physical):
            left = site[k, :, s].reshape(rows * height, site.shape[-1])
            total += lax.dot_general(
                left,
                moved[:, s * block : (s + 1) * block],
                (((0,), (0,)), ((), ())),
                preferred_element_type=jnp.float32,
            )
        out[k] = total.astype(jnp.bfloat16)


def shards(intersect_left, stored_block, stored_site, current_site, current_block, penalty_weight):
    states = lax.axis_size(STATE)
    rows = lax.axis_size(ROW)
    pairs, width, bond = stored_block.shape[1:]
    physical = stored_site.shape[1]
    block = current_block.shape[2]
    slots = 4
    count = pairs * width
    height = 2 * width
    half = block // 2
    group = (*STATE, NEAR, CORE)
    anywhere = pl.BlockSpec(memory_space=pl.ANY)
    resident = pl.BlockSpec(memory_space=pltpu.VMEM)

    turned = current_block.reshape(count, block).T.reshape(2, slots, width, count)
    turned = turned.transpose(1, 0, 2, 3).reshape(slots, height, count)
    turned = jnp.broadcast_to(turned, (states, *turned.shape)).reshape(-1, height, count)
    with jax.named_scope("current"):
        current = exchanged(turned, group).reshape(states, slots, height, count)

    site = current_site.reshape(width, physical, 2, half).transpose(2, 1, 0, 3)
    with jax.named_scope("site_a"):
        site = exchanged(site, FAR)
    site = site.transpose(1, 0, 2, 3).reshape(physical, height, half)
    with jax.named_scope("site_b"):
        site = sent_to_all(site, ROW)
    with jax.named_scope("site_c"):
        site = sent_to_all(site, STATE)

    mine = intersect_left[0]
    with jax.named_scope("pair"):
        other = shifted(mine, FAR, 1)
    first = lax.axis_index(FAR) == 0
    environment = jnp.where(first, jnp.stack([mine, other]), jnp.stack([other, mine]))
    environment = environment.reshape(height, bond)
    pieces = [environment]
    below = above = environment
    for step in range(1, rows // 2):
        with jax.named_scope(f"up_{step}"):
            below = shifted(below, ROW, 1)
        with jax.named_scope(f"down_{step}"):
            above = shifted(above, ROW, -1)
        pieces += [below, above]
    with jax.named_scope(f"up_{rows // 2}"):
        low = shifted(below[:width], ROW, 1)
    with jax.named_scope(f"down_{rows // 2}"):
        high = shifted(above[width:], ROW, -1)
    pieces += [low, high]

    stored = stored_block[0].reshape(count, bond)
    with jax.named_scope("stored_core"):
        stored_core = shifted(stored, CORE, 1)
    with jax.named_scope("stored_near"):
        stored_near = shifted(after(stored, other), NEAR, 1)
    with jax.named_scope("stored_both"):
        stored_both = shifted(stored_near, CORE, 1)

    column = (FAR, NEAR)
    local = after(stored_site[0].reshape(physical * width, bond), stored_near)
    with jax.named_scope("left_1"):
        left = shifted(local, column, 1)
    with jax.named_scope("right_1"):
        right = shifted(local, column, -1)
    left_rows, right_rows = left[:width], right[width:]
    with jax.named_scope("left_2"):
        left_far = shifted(left_rows, column, 1)
    with jax.named_scope("right_2"):
        right_far = shifted(right_rows, column, -1)
    local = jnp.concatenate([local, left, right, left_far, right_far])
    with jax.named_scope("site_core"):
        across = shifted(local, CORE, 1)
    local = local.reshape(4, physical, width, bond)
    across = across.reshape(4, physical, width, bond)

    projected, overlap = pl.pallas_call(
        project_kernel,
        out_shape=(
            jax.ShapeDtypeStruct((rows, slots, height, count), jnp.bfloat16),
            jax.ShapeDtypeStruct((8, 128), jnp.float32),
        ),
        in_specs=[anywhere] * 13 + [resident],
        out_specs=(resident, resident),
        scratch_shapes=[
            pltpu.VMEM((rows, height, bond), jnp.bfloat16),
            pltpu.VMEM((slots, count, bond), jnp.bfloat16),
            pltpu.SemaphoreType.DMA((13,)),
        ],
        cost_estimate=pl.CostEstimate(flops=2 * 512 * 512 * 2048, bytes_accessed=5 << 20, transcendentals=0),
        name="project",
    )(*pieces, stored, stored_near, stored_core, stored_both, current)

    with jax.named_scope("projected"):
        received = exchanged(projected.reshape(-1, height, count), group)
    received = received.reshape(states, slots, height, count)

    with jax.named_scope("sum_a"):
        total = exchanged(jnp.broadcast_to(overlap[:1], (states * slots, 1, 128)), group)
    total = total.reshape(states, slots, 128).sum(axis=1)
    with jax.named_scope("sum_b"):
        total = sent_to_all(total, (ROW, FAR))
    intersect = total.sum(axis=0)[:, 0] * (1.0 / (physical * bond))

    grown = pl.pallas_call(
        grow_kernel,
        out_shape=jax.ShapeDtypeStruct((states, half, block), jnp.bfloat16),
        in_specs=[anywhere] * 11 + [resident],
        out_specs=resident,
        scratch_shapes=[
            pltpu.VMEM((rows, height, bond), jnp.bfloat16),
            pltpu.VMEM((physical, 8, width, bond), jnp.bfloat16),
            pltpu.VMEM((rows * height, physical * block), jnp.bfloat16),
            pltpu.SemaphoreType.DMA((25,)),
        ],
        cost_estimate=pl.CostEstimate(flops=3 * 512 * 512 * 2048, bytes_accessed=6 << 20, transcendentals=0),
        name="grow",
    )(*pieces, local, across, site)

    with jax.named_scope("grown"):
        grown = exchanged(grown.reshape(states * slots, width, block), (ROW, NEAR, CORE))
    grown = grown.reshape(rows, slots, width, block).astype(jnp.float32).sum(axis=1)
    intersect_next = grown.astype(jnp.bfloat16).transpose(1, 0, 2).reshape(1, width, rows * block)

    gain = penalty_weight * intersect
    summed = jnp.sum(gain[:, None, None, None] * received.astype(jnp.float32), axis=0)
    summed = summed.reshape(slots, 2, width, count).transpose(1, 0, 2, 3).reshape(block, count)
    penalized = current_block.astype(jnp.float32) + summed.T.reshape(pairs, width, block)
    return (penalized, intersect_next)


def solution(mesh):
    torus = Mesh(
        mesh.devices.reshape(2, mesh.shape["state"] // 2, 8, 2, 2, 2),
        (*STATE, ROW, FAR, NEAR, CORE),
    )
    bond = (ROW, FAR, NEAR, CORE)
    in_specs = (
        P(STATE, bond, None),
        P(STATE, None, bond, None),
        P(STATE, None, bond, None),
        P(bond, None, STATE),
        P(None, bond, STATE),
        P(),
    )
    out_specs = (P(None, bond, STATE), P(STATE, bond, None))
    return jax.shard_map(
        shards, mesh=torus, in_specs=in_specs, out_specs=out_specs, check_vma=False
    )
```

```python
import jax
import jax.numpy as jnp
from jax import lax
from jax.experimental import pallas as pl
from jax.experimental.pallas import tpu as pltpu
from jax.sharding import Mesh
from jax.sharding import PartitionSpec as P

STATE = ("state_0", "state_1")
ROW = "bond_0"
FAR = "bond_1"
NEAR = "bond_2"
CORE = "bond_3"


ORDER = (0, 1, 7, 6, 2, 5, 3, 4)


def shifted(value, axis, step):
    size = lax.axis_size(axis)
    return lax.ppermute(value, axis, [(i, (i + step) % size) for i in range(size)])


def exchanged(value, axis):
    return lax.all_to_all(value, axis, split_axis=0, concat_axis=0, tiled=True)


def sent_to_all(value, axis):
    return exchanged(jnp.broadcast_to(value, (lax.axis_size(axis), *value.shape)), axis)


def after(value, *others):
    return lax.optimization_barrier((value, *others))[0]


def load_environment(pieces, environment, semaphores):
    rows = environment.shape[0]
    z = lax.axis_index(ROW)
    copies = []

    def load(piece, offset, target=None):
        place = environment.at[lax.rem(z + offset, rows)]
        if target is not None:
            place = place.at[target]
        copies.append(pltpu.make_async_copy(piece, place, semaphores.at[len(copies)]))

    *whole, low, high = pieces
    load(whole[0], 0)
    for step in range(1, rows // 2):
        load(whole[2 * step - 1], rows - step)
        load(whole[2 * step], step)
    split = low.shape[0]
    load(low, rows // 2, pl.ds(0, split))
    load(high, rows // 2, pl.ds(split, split))
    for copy in copies:
        copy.start()
    return copies


def rows_times(left, right):
    return lax.dot_general(left, right, (((1,), (1,)), ((), ())), preferred_element_type=jnp.float32)


def project_kernel(*refs):
    pieces = refs[:9]
    stored = refs[9:13]
    current, out, environment, operand, semaphores = refs[13:]
    v = lax.axis_index(NEAR)
    c = lax.axis_index(CORE)
    copies = []
    for k, (flip_v, flip_c) in enumerate(((0, 0), (1, 0), (0, 1), (1, 1))):
        slot = lax.rem(v + flip_v, 2) * 2 + lax.rem(c + flip_c, 2)
        copies.append(pltpu.make_async_copy(stored[k], operand.at[slot], semaphores.at[9 + k]))
        copies[-1].start()
    copies += load_environment(pieces, environment, semaphores)
    for copy in copies[:4]:
        copy.wait()
    arrived = ((0, 2), (1, 3), (4, 5), (6, 7, 8))
    slots, count, bond = operand.shape
    right = operand[...].reshape(slots * count, bond)
    rows, height, _ = environment.shape
    z = lax.axis_index(ROW)
    total = jnp.zeros((height, count), jnp.float32)
    for step, ready in enumerate(arrived):
        for k in ready:
            copies[4 + k].wait()
        places = [lax.rem(z + offset, rows) for offset in ORDER[2 * step : 2 * step + 2]]
        left = jnp.concatenate([environment[place] for place in places])
        product = rows_times(left, right)
        for i, place in enumerate(places):
            for k in range(slots):
                one = product[i * height : (i + 1) * height, k * count : (k + 1) * count]
                out[place, k, :height] = one.astype(jnp.bfloat16)
                total += one * current[place, k].astype(jnp.float32)
    whole = jnp.full((8, count), jnp.sum(total), jnp.float32)
    high = whole.astype(jnp.bfloat16).astype(jnp.float32)
    middle = (whole - high).astype(jnp.bfloat16).astype(jnp.float32)
    low = whole - high - middle
    row = lax.broadcasted_iota(jnp.int32, whole.shape, 0)
    parts = jnp.where(row == 0, high, jnp.where(row == 1, middle, jnp.where(row == 2, low, 0.0)))
    for i in range(rows):
        for k in range(slots):
            out[i, k, height:] = parts.astype(jnp.bfloat16)


def grow_kernel(*refs):
    pieces = refs[:9]
    mine, other, site, out, environment, operand, moved, semaphores = refs[9:]
    y = lax.axis_index(FAR) * 2 + lax.axis_index(NEAR)
    c = lax.axis_index(CORE)
    copies = load_environment(pieces, environment, semaphores)
    number = len(copies)
    for k, offset in enumerate((0, 3, 1, 2)):
        for flip, source in enumerate((mine, other)):
            slot = lax.rem(y + offset, 4) * 2 + lax.rem(c + flip, 2)
            for s in range(operand.shape[0]):
                copy = pltpu.make_async_copy(
                    source.at[k, s], operand.at[s, slot], semaphores.at[number]
                )
                copy.start()
                copies.append(copy)
                number += 1
    for copy in copies:
        copy.wait()
    physical, slots, count, bond = operand.shape
    block = slots * count
    right = operand[...].reshape(physical * block, bond)
    rows, height, _ = environment.shape
    for z in range(0, rows, 2):
        left = environment[z : z + 2].reshape(2 * height, bond)
        moved[z * height : (z + 2) * height] = rows_times(left, right).astype(jnp.bfloat16)
    for k in range(out.shape[0]):
        total = jnp.zeros(out.shape[1:], jnp.float32)
        for s in range(physical):
            left = site[k, :, s].reshape(rows * height, site.shape[-1])
            total += lax.dot_general(
                left,
                moved[:, s * block : (s + 1) * block],
                (((0,), (0,)), ((), ())),
                preferred_element_type=jnp.float32,
            )
        out[k] = total.astype(jnp.bfloat16)


def whole(intersect_left, stored_block, stored_site, current_site, current_block, penalty_weight):
    states = lax.axis_size(STATE)
    rows = lax.axis_size(ROW)
    pairs, width, bond = stored_block.shape[1:]
    physical = stored_site.shape[1]
    block = current_block.shape[2]
    slots = 4
    count = pairs * width
    height = 2 * width
    half = block // 2
    group = (*STATE, NEAR, CORE)
    anywhere = pl.BlockSpec(memory_space=pl.ANY)
    resident = pl.BlockSpec(memory_space=pltpu.VMEM)

    turned = current_block.reshape(count, block).T.reshape(2, slots, width, count)
    turned = turned.transpose(1, 0, 2, 3).reshape(slots, height, count)
    turned = jnp.broadcast_to(turned, (states, *turned.shape)).reshape(-1, height, count)
    current = exchanged(turned, group).reshape(states, slots, height, count)

    site = current_site.reshape(width, physical, 2, half).transpose(2, 1, 0, 3)
    first = lax.axis_index(FAR) == 0
    kept = jnp.where(first, site[0], site[1])
    got = shifted(jnp.where(first, site[1], site[0]), FAR, 1)
    site = jnp.where(first, jnp.stack([kept, got]), jnp.stack([got, kept]))
    site = site.transpose(1, 0, 2, 3).reshape(physical, height, half)
    site = sent_to_all(site, ROW)
    site = sent_to_all(site, STATE)

    mine = intersect_left[0]
    other = shifted(mine, FAR, 1)
    environment = jnp.where(first, jnp.stack([mine, other]), jnp.stack([other, mine]))
    environment = environment.reshape(height, bond)
    pieces = [environment]
    below = above = environment
    for _ in range(1, rows // 2):
        below = shifted(below, ROW, 1)
        above = shifted(above, ROW, -1)
        pieces += [below, above]
    low = shifted(below[:width], ROW, 1)
    high = shifted(above[width:], ROW, -1)
    pieces += [low, high]

    stored = stored_block[0].reshape(count, bond)
    stored_core = shifted(stored, CORE, 1)
    stored_near = shifted(after(stored, other), NEAR, 1)
    stored_both = shifted(stored_near, CORE, 1)

    column = (FAR, NEAR)
    local = after(stored_site[0].reshape(physical * width, bond), stored_near)
    left = shifted(local, column, 1)
    right = shifted(local, column, -1)
    left_rows, right_rows = left[:width], right[width:]
    left_far = shifted(left_rows, column, 1)
    right_far = shifted(right_rows, column, -1)
    local = jnp.concatenate([local, left, right, left_far, right_far])
    across = shifted(local, CORE, 1)
    local = local.reshape(4, physical, width, bond)
    across = across.reshape(4, physical, width, bond)

    projected = pl.pallas_call(
        project_kernel,
        out_shape=jax.ShapeDtypeStruct((rows, slots, height + 8, count), jnp.bfloat16),
        in_specs=[anywhere] * 13 + [resident],
        out_specs=resident,
        scratch_shapes=[
            pltpu.VMEM((rows, height, bond), jnp.bfloat16),
            pltpu.VMEM((slots, count, bond), jnp.bfloat16),
            pltpu.SemaphoreType.DMA((13,)),
        ],
        cost_estimate=pl.CostEstimate(flops=2 * 512 * 512 * 2048, bytes_accessed=5 << 20, transcendentals=0),
        name="project",
    )(*pieces, stored, stored_near, stored_core, stored_both, current)

    received = exchanged(projected.reshape(-1, height + 8, count), group)
    received = received.reshape(states, slots, height + 8, count).astype(jnp.float32)
    total = received[:, :, height : height + 3].sum(axis=(1, 2))
    total = sent_to_all(total, (ROW, FAR))
    intersect = total.sum(axis=0)[:, 0] * (1.0 / (physical * bond))

    grown = pl.pallas_call(
        grow_kernel,
        out_shape=jax.ShapeDtypeStruct((states, half, block), jnp.bfloat16),
        in_specs=[anywhere] * 11 + [resident],
        out_specs=resident,
        scratch_shapes=[
            pltpu.VMEM((rows, height, bond), jnp.bfloat16),
            pltpu.VMEM((physical, 8, width, bond), jnp.bfloat16),
            pltpu.VMEM((rows * height, physical * block), jnp.bfloat16),
            pltpu.SemaphoreType.DMA((25,)),
        ],
        cost_estimate=pl.CostEstimate(flops=3 * 512 * 512 * 2048, bytes_accessed=6 << 20, transcendentals=0),
        name="grow",
    )(*pieces, local, across, site)

    grown = exchanged(grown.reshape(states * slots, width, block), (ROW, NEAR, CORE))
    grown = grown.reshape(rows, slots, width, block).astype(jnp.float32).sum(axis=1)
    intersect_next = grown.astype(jnp.bfloat16).transpose(1, 0, 2).reshape(1, width, rows * block)

    gain = penalty_weight * intersect
    summed = jnp.sum(gain[:, None, None, None] * received[:, :, :height], axis=0)
    summed = summed.reshape(slots, 2, width, count).transpose(1, 0, 2, 3).reshape(block, count)
    penalized = current_block.astype(jnp.float32) + summed.T.reshape(pairs, width, block)
    return (penalized, intersect_next)


def solution(mesh):
    torus = Mesh(
        mesh.devices.reshape(2, mesh.shape["state"] // 2, 8, 2, 2, 2),
        (*STATE, ROW, FAR, NEAR, CORE),
    )
    bond = (ROW, FAR, NEAR, CORE)
    in_specs = (
        P(STATE, bond, None),
        P(STATE, None, bond, None),
        P(STATE, None, bond, None),
        P(bond, None, STATE),
        P(None, bond, STATE),
        P(),
    )
    out_specs = (P(None, bond, STATE), P(STATE, bond, None))
    return jax.shard_map(whole, mesh=torus, in_specs=in_specs, out_specs=out_specs, check_vma=False)
```

```python
import jax
import jax.numpy as jnp
from jax import lax
from jax.experimental import pallas as pl
from jax.experimental.pallas import tpu as pltpu
from jax.sharding import Mesh
from jax.sharding import PartitionSpec as P

STATE = ("state_0", "state_1")
ROW = "bond_0"
FAR = "bond_1"
NEAR = "bond_2"
CORE = "bond_3"


ORDER = (0, 7, 1, 6, 2, 5, 3, 4)


def shifted(value, axis, step):
    size = lax.axis_size(axis)
    return lax.ppermute(value, axis, [(i, (i + step) % size) for i in range(size)])


def exchanged(value, axis):
    return lax.all_to_all(value, axis, split_axis=0, concat_axis=0, tiled=True)


def sent_to_all(value, axis):
    return exchanged(jnp.broadcast_to(value, (lax.axis_size(axis), *value.shape)), axis)


def rows_times(left, right):
    return lax.dot_general(left, right, (((1,), (1,)), ((), ())), preferred_element_type=jnp.float32)


def paired(pieces):
    for step in range(0, len(ORDER), 2):
        left = jnp.concatenate([piece[...] for piece in pieces[step : step + 2]])
        yield left, ORDER[step : step + 2]


def join_kernel(*refs):
    *pieces, out = refs
    for k, piece in enumerate(pieces):
        out[k] = piece[...]


def joined(*pieces):
    resident = pl.BlockSpec(memory_space=pltpu.VMEM)
    return pl.pallas_call(
        join_kernel,
        out_shape=jax.ShapeDtypeStruct((len(pieces), *pieces[0].shape), pieces[0].dtype),
        in_specs=[resident] * len(pieces),
        out_specs=resident,
    )(*pieces)


def project_kernel(*refs):
    pieces = refs[:8]
    stored = refs[8:10]
    spread, out = refs[10:]
    z = lax.axis_index(ROW)
    v = lax.axis_index(NEAR)
    c = lax.axis_index(CORE)
    height, count = spread.shape[3:]
    rows, slots = out.shape[:2]
    wide = spread.shape[0]
    behind = spread.shape[2] - slots
    right = jnp.concatenate([piece[...] for piece in stored])
    targets = [
        lax.rem(v + flip_v, 2) * 2 + lax.rem(c + flip_c, 2)
        for flip_v, flip_c in ((0, 0), (1, 0), (0, 1), (1, 1))
    ]
    total = jnp.zeros((height, count), jnp.float32)
    for left, offsets in paired(pieces):
        product = rows_times(left, right)
        for i, offset in enumerate(offsets):
            place = lax.rem(z + offset, rows)
            for k, target in enumerate(targets):
                one = product[i * height : (i + 1) * height, k * count : (k + 1) * count]
                out[place, target, :height] = one.astype(jnp.bfloat16)
                current = spread[lax.rem(place, wide), place // wide, behind + target]
                total += one * current.astype(jnp.float32)
    whole = jnp.full((8, count), jnp.sum(total), jnp.float32)
    high = whole.astype(jnp.bfloat16).astype(jnp.float32)
    middle = (whole - high).astype(jnp.bfloat16).astype(jnp.float32)
    low = whole - high - middle
    row = lax.broadcasted_iota(jnp.int32, whole.shape, 0)
    parts = jnp.where(row == 0, high, jnp.where(row == 1, middle, jnp.where(row == 2, low, 0.0)))
    for i in range(rows):
        for k in range(slots):
            out[i, k, height:] = parts.astype(jnp.bfloat16)


def grow_kernel(*refs):
    pieces = refs[:8]
    mine, other, spread, keep, give, operand, moved, semaphores = refs[8:]
    z = lax.axis_index(ROW)
    y = lax.axis_index(FAR) * 2 + lax.axis_index(NEAR)
    c = lax.axis_index(CORE)
    copies = []
    for k, offset in enumerate((0, 3, 1, 2)):
        for flip, source in enumerate((mine, other)):
            slot = lax.rem(y + offset, 4) * 2 + lax.rem(c + flip, 2)
            for s in range(operand.shape[0]):
                copy = pltpu.make_async_copy(
                    source.at[k, s], operand.at[s, slot], semaphores.at[len(copies)]
                )
                copy.start()
                copies.append(copy)
    for copy in copies:
        copy.wait()
    physical, slots, count, bond = operand.shape
    block = slots * count
    height, half = spread.shape[3:]
    rows = moved.shape[0]
    wide = spread.shape[0]
    right = operand[...].reshape(physical * block, bond)
    for left, offsets in paired(pieces):
        product = rows_times(left, right).astype(jnp.bfloat16)
        for i, offset in enumerate(offsets):
            moved[lax.rem(z + offset, rows)] = product[i * height : (i + 1) * height]
    inner = moved[...].reshape(rows * height, physical * block)
    for k in range(keep.shape[0]):
        total = jnp.zeros((half, block), jnp.float32)
        for s in range(physical):
            left = spread[k % wide, k // wide, s * rows : (s + 1) * rows]
            total += lax.dot_general(
                left.reshape(rows * height, half),
                inner[:, s * block : (s + 1) * block],
                (((0,), (0,)), ((), ())),
                preferred_element_type=jnp.float32,
            )
        for i in range(2):
            first = total[2 * i * count : (2 * i + 1) * count]
            second = total[(2 * i + 1) * count : (2 * i + 2) * count]
            keep[k, i] = jnp.where(c == 0, first, second).astype(jnp.bfloat16)
            give[k, i] = jnp.where(c == 0, second, first).astype(jnp.bfloat16)


def whole(intersect_left, stored_block, stored_site, current_site, current_block, penalty_weight):
    states = lax.axis_size(STATE)
    rows = lax.axis_size(ROW)
    pairs, width, bond = stored_block.shape[1:]
    physical = stored_site.shape[1]
    block = current_block.shape[2]
    slots = 4
    count = pairs * width
    height = 2 * width
    half = block // 2
    group = (*STATE, NEAR, CORE)
    anywhere = pl.BlockSpec(memory_space=pl.ANY)
    resident = pl.BlockSpec(memory_space=pltpu.VMEM)

    both = jnp.concatenate(
        [current_block.reshape(count, block), current_site.reshape(width * physical, block)]
    )
    across = shifted(both, STATE[0], 1)
    low = lax.axis_index(STATE[0]) == 0
    both = jnp.where(low, jnp.stack([both, across]), jnp.stack([across, both]))

    turned = both[:, :count].transpose(0, 2, 1).reshape(2, 2, slots, width, count)
    turned = turned.transpose(2, 0, 1, 3, 4).reshape(slots, 2, height, count)
    current = exchanged(turned, (NEAR, CORE)).transpose(1, 0, 2, 3)

    first = lax.axis_index(FAR) == 0
    mine = intersect_left[0]
    site = both[:, count:].reshape(2, width, physical, block).transpose(1, 0, 2, 3)
    site = site.reshape(width, 2 * physical, block)
    kept = jnp.where(first, site[:, :, :half], site[:, :, half:]).reshape(width, -1)
    given = jnp.where(first, site[:, :, half:], site[:, :, :half]).reshape(width, -1)
    other = shifted(jnp.concatenate([mine, given], axis=1), FAR, 1)
    got = other[:, bond:]
    other = other[:, :bond]
    site = jnp.where(first, jnp.stack([kept, got]), jnp.stack([got, kept]))
    site = site.reshape(height, 2 * physical, half).transpose(1, 0, 2)
    site = sent_to_all(site, ROW)
    site = site.transpose(1, 0, 2, 3).reshape(2, physical * rows, height, half)
    spread = sent_to_all(jnp.concatenate([site, current], axis=1), STATE[1])
    environment = jnp.where(first, jnp.stack([mine, other]), jnp.stack([other, mine]))
    environment = environment.reshape(height, bond)
    pieces = [environment]
    below = above = environment
    for _ in range(1, rows // 2):
        below = shifted(below, ROW, 1)
        above = shifted(above, ROW, -1)
        pieces += [below, above]
    pieces.append(shifted(below, ROW, 1))

    column = (FAR, NEAR)
    local = stored_site[0].reshape(physical * width, bond)
    left = shifted(local, column, 1)
    right = shifted(local, column, -1)
    opposite = shifted(local, FAR, 1)
    local = joined(local, left, right, opposite)
    across = shifted(local, CORE, 1)
    local = local.reshape(4, physical, width, bond)
    across = across.reshape(4, physical, width, bond)

    stored = stored_block[0].reshape(count, bond)
    stored_near = shifted(stored, NEAR, 1)
    stored_pair = joined(stored, stored_near).reshape(2 * count, bond)
    stored_other = shifted(stored_pair, CORE, 1)

    projected = pl.pallas_call(
        project_kernel,
        out_shape=jax.ShapeDtypeStruct((rows, slots, height + 8, count), jnp.bfloat16),
        in_specs=[resident] * 11,
        out_specs=resident,
        cost_estimate=pl.CostEstimate(flops=2 * 512 * 512 * 2048, bytes_accessed=5 << 20, transcendentals=0),
        name="project",
    )(*pieces, stored_pair, stored_other, spread)


    received = exchanged(projected.reshape(-1, height + 8, count), group)
    received = received.reshape(states, slots, height + 8, count).astype(jnp.float32)
    total = received[:, :, height : height + 3].sum(axis=(1, 2))
    total = total + shifted(total, FAR, 1)

    keep, give = pl.pallas_call(
        grow_kernel,
        out_shape=(jax.ShapeDtypeStruct((states, 2, width, block), jnp.bfloat16),) * 2,
        in_specs=[resident] * 8 + [anywhere] * 2 + [resident],
        out_specs=(resident, resident),
        scratch_shapes=[
            pltpu.VMEM((physical, 8, width, bond), jnp.bfloat16),
            pltpu.VMEM((rows, height, physical * block), jnp.bfloat16),
            pltpu.SemaphoreType.DMA((16,)),
        ],
        cost_estimate=pl.CostEstimate(flops=3 * 512 * 512 * 2048, bytes_accessed=6 << 20, transcendentals=0),
        name="grow",
    )(*pieces, local, across, spread)
    got = shifted(give, CORE, 1)
    grown = (keep.astype(jnp.float32) + got.astype(jnp.float32)).astype(jnp.bfloat16)

    total = jnp.broadcast_to(total[:, :1], (states, block))
    high = lax.reduce_precision(total, 8, 7)
    middle = lax.reduce_precision(total - high, 8, 7)
    low = total - high - middle
    lane = lax.broadcasted_iota(jnp.int32, total.shape, 1)
    parts = jnp.where(lane == 0, high, jnp.where(lane == 1, middle, jnp.where(lane == 2, low, 0.0)))
    parts = parts.astype(jnp.bfloat16)[:, None]
    parts = jnp.broadcast_to(parts.reshape(1, 1, states, block), (states, 2, 8, block))
    grown = jnp.concatenate([grown, parts], axis=2).reshape(states * 2, width + 8, block)
    grown = exchanged(grown, (ROW, NEAR))
    grown = grown.reshape(rows, 2, width + 8, block).astype(jnp.float32)
    intersect = grown[:, 0, width:, :3].sum(axis=(0, 2)) * (1.0 / (physical * bond))
    grown = grown[:, :, :width].sum(axis=1)
    intersect_next = grown.astype(jnp.bfloat16).transpose(1, 0, 2).reshape(1, width, rows * block)

    gain = penalty_weight * intersect
    summed = jnp.sum(gain[:, None, None, None] * received[:, :, :height], axis=0)
    summed = summed.reshape(slots, 2, width, count).transpose(1, 0, 2, 3).reshape(block, count)
    penalized = current_block.astype(jnp.float32) + summed.T.reshape(pairs, width, block)
    return (penalized, intersect_next)


def solution(mesh):
    torus = Mesh(
        mesh.devices.reshape(2, mesh.shape["state"] // 2, 8, 2, 2, 2),
        (*STATE, ROW, FAR, NEAR, CORE),
    )
    bond = (ROW, FAR, NEAR, CORE)
    in_specs = (
        P(STATE, bond, None),
        P(STATE, None, bond, None),
        P(STATE, None, bond, None),
        P(bond, None, STATE),
        P(None, bond, STATE),
        P(),
    )
    out_specs = (P(None, bond, STATE), P(STATE, bond, None))
    return jax.shard_map(whole, mesh=torus, in_specs=in_specs, out_specs=out_specs, check_vma=False)
```

```python
import jax
import jax.numpy as jnp
from jax import lax
from jax.experimental import pallas as pl
from jax.experimental.pallas import tpu as pltpu
from jax.sharding import Mesh
from jax.sharding import PartitionSpec as P

STATE = ("state_0", "state_1")
ROW = "bond_0"
FAR = "bond_1"
NEAR = "bond_2"
CORE = "bond_3"


ORDER = (0, 7, 1, 6, 2, 5, 3, 4)


def shifted(value, axis, step):
    size = lax.axis_size(axis)
    return lax.ppermute(value, axis, [(i, (i + step) % size) for i in range(size)])


def exchanged(value, axis):
    return lax.all_to_all(value, axis, split_axis=0, concat_axis=0, tiled=True)


def sent_to_all(value, axis):
    return exchanged(jnp.broadcast_to(value, (lax.axis_size(axis), *value.shape)), axis)


def rows_times(left, right):
    return lax.dot_general(left, right, (((1,), (1,)), ((), ())), preferred_element_type=jnp.float32)


def paired(pieces):
    for step in range(0, len(ORDER), 2):
        last = len(pieces) if step + 2 == len(ORDER) else step + 2
        left = jnp.concatenate([piece[...] for piece in pieces[step:last]])
        yield left, ORDER[step : step + 2]


def join_kernel(*refs):
    *pieces, out = refs
    for k, piece in enumerate(pieces):
        out[k] = piece[...]


def joined(*pieces):
    resident = pl.BlockSpec(memory_space=pltpu.VMEM)
    return pl.pallas_call(
        join_kernel,
        out_shape=jax.ShapeDtypeStruct((len(pieces), *pieces[0].shape), pieces[0].dtype),
        in_specs=[resident] * len(pieces),
        out_specs=resident,
    )(*pieces)


def project_kernel(*refs):
    pieces = refs[:9]
    mine, other, seen, out = refs[9:]
    z = lax.axis_index(ROW)
    c = lax.axis_index(CORE)
    height, count = seen.shape[2:]
    rows, cores = out.shape[:2]
    right = jnp.concatenate([mine[...], other[...]])
    total = jnp.zeros((height, count), jnp.float32)
    for left, offsets in paired(pieces):
        product = rows_times(left, right)
        for i, offset in enumerate(offsets):
            place = lax.rem(z + offset, rows)
            for k in range(cores):
                target = lax.rem(c + k, cores)
                one = product[i * height : (i + 1) * height, k * count : (k + 1) * count]
                out[place, target, :height] = one.astype(jnp.bfloat16)
                current = seen[place, target]
                total += one * current.astype(jnp.float32)
    whole = jnp.full((8, count), jnp.sum(total), jnp.float32)
    high = whole.astype(jnp.bfloat16).astype(jnp.float32)
    middle = (whole - high).astype(jnp.bfloat16).astype(jnp.float32)
    low = whole - high - middle
    row = lax.broadcasted_iota(jnp.int32, whole.shape, 0)
    parts = jnp.where(row == 0, high, jnp.where(row == 1, middle, jnp.where(row == 2, low, 0.0)))
    for i in range(rows):
        for k in range(cores):
            out[i, k, height:] = parts.astype(jnp.bfloat16)


def grow_kernel(*refs):
    pieces = refs[:9]
    stored = refs[9:13]
    spread, keep, give, operand, moved, semaphores = refs[13:]
    z = lax.axis_index(ROW)
    u = lax.axis_index(FAR)
    v = lax.axis_index(NEAR)
    c = lax.axis_index(CORE)
    copies = []
    for k, source in enumerate(stored):
        for near in range(2):
            column = lax.rem(u + k % 2, 2) * 2 + lax.rem(v + k % 2 + near, 2)
            slot = column * 2 + lax.rem(c + k // 2, 2)
            for s in range(operand.shape[0]):
                copy = pltpu.make_async_copy(
                    source.at[near, s], operand.at[s, slot], semaphores.at[len(copies)]
                )
                copy.start()
                copies.append(copy)
    for copy in copies:
        copy.wait()
    physical, slots, width, bond = operand.shape
    block = slots * width
    rows, height, _ = moved.shape
    wide = spread.shape[0]
    lanes = spread.shape[4]
    part = lanes // physical
    right = operand[...].reshape(physical * block, bond)
    for left, offsets in paired(pieces):
        product = rows_times(left, right).astype(jnp.bfloat16)
        for i, offset in enumerate(offsets):
            moved[lax.rem(z + offset, rows)] = product[i * height : (i + 1) * height]
    inner = moved[...].reshape(rows * height, physical * block)
    for k in range(keep.shape[0]):
        left = spread[k % wide, k // wide].reshape(rows * height, lanes)
        crossed = lax.dot_general(
            left, inner, (((0,), (0,)), ((), ())), preferred_element_type=jnp.float32
        )
        total = crossed[:part, :block]
        for s in range(1, physical):
            total += crossed[s * part : (s + 1) * part, s * block : (s + 1) * block]
        first, second = total[:width], total[width:]
        keep[k] = jnp.where(c == 0, first, second)
        give[k] = jnp.where(c == 0, second, first).astype(jnp.bfloat16)


def whole(intersect_left, stored_block, stored_site, current_site, current_block, penalty_weight):
    states = lax.axis_size(STATE)
    rows = lax.axis_size(ROW)
    pairs, width, bond = stored_block.shape[1:]
    physical = stored_site.shape[1]
    block = current_block.shape[2]
    columns = 4
    count = pairs * width
    height = columns * width
    part = block // columns
    column = (FAR, NEAR)
    group = (*STATE, CORE)
    anywhere = pl.BlockSpec(memory_space=pl.ANY)
    resident = pl.BlockSpec(memory_space=pltpu.VMEM)

    mine = intersect_left[0]
    other = shifted(mine, NEAR, 1)
    first = lax.axis_index(NEAR) == 0
    mine = jnp.where(first, jnp.stack([mine, other]), jnp.stack([other, mine]))
    other = lax.ppermute(mine, column, [(i, 3 - i) for i in range(4)])
    first = lax.axis_index(FAR) == 0
    environment = jnp.where(first, jnp.stack([mine, other]), jnp.stack([other, mine]))
    environment = environment.reshape(height, bond)

    site = current_site.reshape(width, physical, columns, part).transpose(2, 0, 1, 3)
    site = exchanged(site.reshape(columns, width, physical * part), column)
    site = site.reshape(height, physical * part)

    site = sent_to_all(site, (STATE[0], ROW))
    spread = sent_to_all(site, STATE[1]).reshape(-1, 2, rows, height, physical * part)

    turned = current_block.reshape(count, block).T.reshape(columns, 2, width, count)
    turned = turned.transpose(1, 0, 2, 3).reshape(2, height, count)
    turned = jnp.broadcast_to(turned, (states, *turned.shape)).reshape(-1, height, count)
    seen = exchanged(turned, group).reshape(states, 2, height, count)

    pieces = [environment]
    below = above = environment
    for _ in range(1, rows // 2):
        below = shifted(below, ROW, 1)
        above = shifted(above, ROW, -1)
        pieces += [below, above]
    pieces.append(shifted(below[: height // 2], ROW, 1))
    pieces.append(shifted(above[height // 2 :], ROW, -1))

    local = stored_site[0].reshape(physical * width, bond)
    site_near = shifted(local, NEAR, 1)
    site_pair = joined(local, site_near).reshape(2, physical, width, bond)
    site_far = lax.ppermute(site_pair, (FAR, NEAR), [(i, 3 - i) for i in range(4)])
    site_pair_other = shifted(site_pair, CORE, 1)
    site_far_other = shifted(site_far, CORE, 1)

    stored = stored_block[0].reshape(count, bond)
    stored_other = shifted(stored, CORE, 1)

    projected = pl.pallas_call(
        project_kernel,
        out_shape=jax.ShapeDtypeStruct((rows, 2, height + 8, count), jnp.bfloat16),
        in_specs=[resident] * 12,
        out_specs=resident,
        cost_estimate=pl.CostEstimate(flops=2 * 512 * 512 * 2048, bytes_accessed=5 << 20, transcendentals=0),
        name="project",
    )(*pieces, stored, stored_other, seen)

    received = exchanged(projected.reshape(-1, height + 8, count), group)
    received = received.reshape(states, 2, height + 8, count).astype(jnp.float32)
    total = received[:, :, height : height + 3].sum(axis=(1, 2))
    total = sent_to_all(total, column).sum(axis=0)

    keep, give = pl.pallas_call(
        grow_kernel,
        out_shape=(
            jax.ShapeDtypeStruct((states, width, block), jnp.float32),
            jax.ShapeDtypeStruct((states, width, block), jnp.bfloat16),
        ),
        in_specs=[resident] * 9 + [anywhere] * 4 + [resident],
        out_specs=(resident, resident),
        scratch_shapes=[
            pltpu.VMEM((physical, 8, width, bond), jnp.bfloat16),
            pltpu.VMEM((rows, height, physical * block), jnp.bfloat16),
            pltpu.SemaphoreType.DMA((16,)),
        ],
        cost_estimate=pl.CostEstimate(flops=3 * 512 * 512 * 2048, bytes_accessed=6 << 20, transcendentals=0),
        name="grow",
    )(*pieces, site_pair, site_far, site_pair_other, site_far_other, spread)
    got = shifted(give, CORE, 1)
    grown = (keep + got.astype(jnp.float32)).astype(jnp.bfloat16)

    total = jnp.broadcast_to(total[:, :1], (states, block))
    high = lax.reduce_precision(total, 8, 7)
    middle = lax.reduce_precision(total - high, 8, 7)
    low = total - high - middle
    lane = lax.broadcasted_iota(jnp.int32, total.shape, 1)
    parts = jnp.where(lane == 0, high, jnp.where(lane == 1, middle, jnp.where(lane == 2, low, 0.0)))
    parts = jnp.broadcast_to(parts.astype(jnp.bfloat16), (states, states, block))
    grown = jnp.concatenate([grown, parts], axis=1)
    grown = exchanged(grown, ROW)
    intersect = grown[:, width:, :3].astype(jnp.float32).sum(axis=(0, 2))
    intersect = intersect * (1.0 / (physical * bond))
    intersect_next = grown[:, :width].transpose(1, 0, 2).reshape(1, width, rows * block)

    gain = penalty_weight * intersect
    summed = jnp.sum(gain[:, None, None, None] * received[:, :, :height], axis=0)
    summed = summed.reshape(2, columns, width, count).transpose(1, 0, 2, 3).reshape(block, count)
    penalized = current_block.astype(jnp.float32) + summed.T.reshape(pairs, width, block)
    return (penalized, intersect_next)


def solution(mesh):
    torus = Mesh(
        mesh.devices.reshape(2, mesh.shape["state"] // 2, 8, 2, 2, 2),
        (*STATE, ROW, FAR, NEAR, CORE),
    )
    bond = (ROW, FAR, NEAR, CORE)
    in_specs = (
        P(STATE, bond, None),
        P(STATE, None, bond, None),
        P(STATE, None, bond, None),
        P(bond, None, STATE),
        P(None, bond, STATE),
        P(),
    )
    out_specs = (P(None, bond, STATE), P(STATE, bond, None))
    return jax.shard_map(whole, mesh=torus, in_specs=in_specs, out_specs=out_specs, check_vma=False)
```

```python
import jax
import jax.numpy as jnp
from jax import lax
from jax.experimental import pallas as pl
from jax.experimental.pallas import tpu as pltpu
from jax.sharding import Mesh
from jax.sharding import PartitionSpec as P

STATE = ("state_0", "state_1")
ROW = "bond_0"
FAR = "bond_1"
NEAR = "bond_2"
CORE = "bond_3"


ORDER = (0, 7, 1, 6, 2, 5, 3, 4)


def shifted(value, axis, step):
    size = lax.axis_size(axis)
    return lax.ppermute(value, axis, [(i, (i + step) % size) for i in range(size)])


def exchanged(value, axis):
    return lax.all_to_all(value, axis, split_axis=0, concat_axis=0, tiled=True)


def sent_to_all(value, axis):
    return exchanged(jnp.broadcast_to(value, (lax.axis_size(axis), *value.shape)), axis)


def rows_times(left, right):
    return lax.dot_general(left, right, (((1,), (1,)), ((), ())), preferred_element_type=jnp.float32)


def paired(pieces):
    for step in range(0, len(ORDER), 2):
        last = len(pieces) if step + 2 == len(ORDER) else step + 2
        left = jnp.concatenate([piece[...] for piece in pieces[step:last]])
        yield left, ORDER[step : step + 2]


def join_kernel(*refs):
    *pieces, out = refs
    for k, piece in enumerate(pieces):
        out[k] = piece[...]


def joined(*pieces):
    resident = pl.BlockSpec(memory_space=pltpu.VMEM)
    return pl.pallas_call(
        join_kernel,
        out_shape=jax.ShapeDtypeStruct((len(pieces), *pieces[0].shape), pieces[0].dtype),
        in_specs=[resident] * len(pieces),
        out_specs=resident,
    )(*pieces)


def project_kernel(*refs):
    pieces = refs[:9]
    mine, other, seen, out = refs[9:]
    z = lax.axis_index(ROW)
    c = lax.axis_index(CORE)
    height, count = seen.shape[2:]
    rows, cores = out.shape[:2]
    right = jnp.concatenate([mine[...], other[...]])
    total = jnp.zeros((height, count), jnp.float32)
    for left, offsets in paired(pieces):
        product = rows_times(left, right)
        for i, offset in enumerate(offsets):
            place = lax.rem(z + offset, rows)
            for k in range(cores):
                target = lax.rem(c + k, cores)
                one = product[i * height : (i + 1) * height, k * count : (k + 1) * count]
                out[place, target, :height] = one.astype(jnp.bfloat16)
                current = seen[place, target]
                total += one * current.astype(jnp.float32)
    whole = jnp.full((8, count), jnp.sum(total), jnp.float32)
    high = whole.astype(jnp.bfloat16).astype(jnp.float32)
    middle = (whole - high).astype(jnp.bfloat16).astype(jnp.float32)
    low = whole - high - middle
    row = lax.broadcasted_iota(jnp.int32, whole.shape, 0)
    parts = jnp.where(row == 0, high, jnp.where(row == 1, middle, jnp.where(row == 2, low, 0.0)))
    for i in range(rows):
        for k in range(cores):
            out[i, k, height:] = parts.astype(jnp.bfloat16)


def grow_kernel(*refs):
    pieces = refs[:9]
    stored = refs[9:13]
    spread, keep, give, operand, moved, semaphores = refs[13:]
    z = lax.axis_index(ROW)
    u = lax.axis_index(FAR)
    v = lax.axis_index(NEAR)
    c = lax.axis_index(CORE)
    copies = []
    for k, source in enumerate(stored):
        for near in range(2):
            column = lax.rem(u + k % 2, 2) * 2 + lax.rem(v + k % 2 + near, 2)
            slot = column * 2 + lax.rem(c + k // 2, 2)
            for s in range(operand.shape[0]):
                copy = pltpu.make_async_copy(
                    source.at[near, s], operand.at[s, slot], semaphores.at[len(copies)]
                )
                copy.start()
                copies.append(copy)
    for copy in copies:
        copy.wait()
    physical, slots, width, bond = operand.shape
    block = slots * width
    rows, height, _ = moved.shape
    wide = spread.shape[0]
    lanes = spread.shape[4]
    part = lanes // physical
    right = operand[...].reshape(physical * block, bond)
    for left, offsets in paired(pieces):
        product = rows_times(left, right).astype(jnp.bfloat16)
        for i, offset in enumerate(offsets):
            moved[lax.rem(z + offset, rows)] = product[i * height : (i + 1) * height]
    inner = moved[...].reshape(rows * height, physical * block)
    for k in range(keep.shape[0]):
        left = spread[k % wide, k // wide].reshape(rows * height, lanes)
        crossed = lax.dot_general(
            left, inner, (((0,), (0,)), ((), ())), preferred_element_type=jnp.float32
        )
        total = crossed[:part, :block]
        for s in range(1, physical):
            total += crossed[s * part : (s + 1) * part, s * block : (s + 1) * block]
        first, second = total[:width], total[width:]
        keep[k] = jnp.where(c == 0, first, second)
        give[k] = jnp.where(c == 0, second, first)


def whole(intersect_left, stored_block, stored_site, current_site, current_block, penalty_weight):
    states = lax.axis_size(STATE)
    rows = lax.axis_size(ROW)
    pairs, width, bond = stored_block.shape[1:]
    physical = stored_site.shape[1]
    block = current_block.shape[2]
    columns = 4
    count = pairs * width
    height = columns * width
    part = block // columns
    column = (FAR, NEAR)
    group = (*STATE, CORE)
    anywhere = pl.BlockSpec(memory_space=pl.ANY)
    resident = pl.BlockSpec(memory_space=pltpu.VMEM)

    mine = intersect_left[0]
    other = shifted(mine, NEAR, 1)
    first = lax.axis_index(NEAR) == 0
    mine = jnp.where(first, jnp.stack([mine, other]), jnp.stack([other, mine]))
    other = lax.ppermute(mine, column, [(i, 3 - i) for i in range(4)])
    first = lax.axis_index(FAR) == 0
    environment = jnp.where(first, jnp.stack([mine, other]), jnp.stack([other, mine]))
    environment = environment.reshape(height, bond)

    site = current_site.reshape(width, physical, columns, part).transpose(2, 0, 1, 3)
    site = exchanged(site.reshape(columns, width, physical * part), column)
    site = site.reshape(height, physical * part)

    site = sent_to_all(site, (STATE[0], ROW))
    spread = sent_to_all(site, STATE[1]).reshape(-1, 2, rows, height, physical * part)

    turned = current_block.reshape(count, block).T.reshape(columns, 2, width, count)
    turned = turned.transpose(1, 0, 2, 3).reshape(2, height, count)
    turned = jnp.broadcast_to(turned, (states, *turned.shape)).reshape(-1, height, count)
    seen = exchanged(turned, group).reshape(states, 2, height, count)

    pieces = [environment]
    below = above = environment
    for _ in range(1, rows // 2):
        below = shifted(below, ROW, 1)
        above = shifted(above, ROW, -1)
        pieces += [below, above]
    pieces.append(shifted(below[: height // 2], ROW, 1))
    pieces.append(shifted(above[height // 2 :], ROW, -1))

    local = stored_site[0].reshape(physical * width, bond)
    site_near = shifted(local, NEAR, 1)
    site_pair = joined(local, site_near).reshape(2, physical, width, bond)
    site_far = lax.ppermute(site_pair, (FAR, NEAR), [(i, 3 - i) for i in range(4)])
    site_pair_other = shifted(site_pair, CORE, 1)
    site_far_other = shifted(site_far, CORE, 1)

    stored = stored_block[0].reshape(count, bond)
    stored_other = shifted(stored, CORE, 1)

    projected = pl.pallas_call(
        project_kernel,
        out_shape=jax.ShapeDtypeStruct((rows, 2, height + 8, count), jnp.bfloat16),
        in_specs=[resident] * 12,
        out_specs=resident,
        cost_estimate=pl.CostEstimate(flops=2 * 512 * 512 * 2048, bytes_accessed=5 << 20, transcendentals=0),
        name="project",
    )(*pieces, stored, stored_other, seen)

    received = exchanged(projected.reshape(-1, height + 8, count), group)
    received = received.reshape(states, 2, height + 8, count).astype(jnp.float32)
    total = received[:, :, height : height + 3].sum(axis=(1, 2))
    total = sent_to_all(total, column).sum(axis=0)

    keep, give = pl.pallas_call(
        grow_kernel,
        out_shape=(
            jax.ShapeDtypeStruct((states, width, block), jnp.float32),
            jax.ShapeDtypeStruct((states, width, block), jnp.float32),
        ),
        in_specs=[resident] * 9 + [anywhere] * 4 + [resident],
        out_specs=(resident, resident),
        scratch_shapes=[
            pltpu.VMEM((physical, 8, width, bond), jnp.bfloat16),
            pltpu.VMEM((rows, height, physical * block), jnp.bfloat16),
            pltpu.SemaphoreType.DMA((16,)),
        ],
        cost_estimate=pl.CostEstimate(flops=3 * 512 * 512 * 2048, bytes_accessed=6 << 20, transcendentals=0),
        name="grow",
    )(*pieces, site_pair, site_far, site_pair_other, site_far_other, spread)
    got = shifted(give, CORE, 1)
    grown = (keep + got).astype(jnp.bfloat16)

    total = jnp.broadcast_to(total[:, :1], (states, block))
    high = lax.reduce_precision(total, 8, 7)
    middle = lax.reduce_precision(total - high, 8, 7)
    low = total - high - middle
    lane = lax.broadcasted_iota(jnp.int32, total.shape, 1)
    parts = jnp.where(lane == 0, high, jnp.where(lane == 1, middle, jnp.where(lane == 2, low, 0.0)))
    parts = jnp.broadcast_to(parts.astype(jnp.bfloat16), (states, states, block))
    grown = jnp.concatenate([grown, parts], axis=1)
    grown = exchanged(grown, ROW)
    intersect = grown[:, width:, :3].astype(jnp.float32).sum(axis=(0, 2))
    intersect = intersect * (1.0 / (physical * bond))
    intersect_next = grown[:, :width].transpose(1, 0, 2).reshape(1, width, rows * block)

    gain = penalty_weight * intersect
    summed = jnp.sum(gain[:, None, None, None] * received[:, :, :height], axis=0)
    summed = summed.reshape(2, columns, width, count).transpose(1, 0, 2, 3).reshape(block, count)
    penalized = current_block.astype(jnp.float32) + summed.T.reshape(pairs, width, block)
    return (penalized, intersect_next)


def solution(mesh):
    torus = Mesh(
        mesh.devices.reshape(2, mesh.shape["state"] // 2, 8, 2, 2, 2),
        (*STATE, ROW, FAR, NEAR, CORE),
    )
    bond = (ROW, FAR, NEAR, CORE)
    in_specs = (
        P(STATE, bond, None),
        P(STATE, None, bond, None),
        P(STATE, None, bond, None),
        P(bond, None, STATE),
        P(None, bond, STATE),
        P(),
    )
    out_specs = (P(None, bond, STATE), P(STATE, bond, None))
    return jax.shard_map(whole, mesh=torus, in_specs=in_specs, out_specs=out_specs, check_vma=False)
```
